128 devices in a mesh: graph: 128 (over z, y, x, core).
Axes of the slice: x: 4, y: 4, z: 4, core: 2. Of those that a mesh axis runs over, the one named last changes fastest.
Arguments:
- node_feats: bfloat16 [524288, 100], P('graph')
- w_one: float32 [100, 256], replicated
- w_two: float32 [256, 47], replicated
- send_idx: int32 [256, 1024], P('graph')
- edge_src: int32 [524288, 4], P('graph')
- edge_w: float32 [524288, 4], P('graph')
- halo_src: int32 [131072, 4], P('graph')
- halo_w: float32 [131072, 4], P('graph')
- labels: int32 [524288], P('graph')
- label_mask: int32 [524288], P('graph')
Outputs:
- output 1: float32 [], replicated
- output 2: float32 [100, 256], replicated
- output 3: float32 [256, 47], replicated
All inputs are finite; a program needn't handle non-finite values.
Results may differ from the reference program's by a relative error of at most 0.001.
Values are sent between devices in bfloat16 or wider.
A program may use at most 1 GiB of HBM per device.

```python
import jax
import jax.numpy as jnp
from jax import lax

NUM_PARTS = 128
NODES_DEV = 4096
HALO_ROWS = 512
DEGREE = 4
CUT_SLOTS = 1
PEERS = 2
FEAT_IN = 100
HIDDEN = 256
CLASSES = 47


def build_graph(graph_key):
    sub_keys = jax.random.split(graph_key, 7)
    band_rows = PEERS * HALO_ROWS
    own_slots = DEGREE - CUT_SLOTS
    orders = jax.vmap(lambda one_key: jax.random.permutation(one_key, NODES_DEV))(jax.random.split(sub_keys[0], NUM_PARTS))
    one_hop = orders[:, :band_rows].reshape(NUM_PARTS, PEERS, HALO_ROWS)
    two_hop = orders[:, band_rows:2 * band_rows].reshape(NUM_PARTS, PEERS, HALO_ROWS)
    send_rows = jnp.concatenate([one_hop, two_hop], axis=2)
    cut_pick = jax.random.randint(sub_keys[1], (NUM_PARTS, PEERS, HALO_ROWS, CUT_SLOTS), 0, HALO_ROWS)
    own_pick = jax.random.randint(sub_keys[2], (NUM_PARTS, PEERS, HALO_ROWS, own_slots), 0, 2 * HALO_ROWS)
    side_col = jnp.arange(PEERS).reshape(1, PEERS, 1, 1)
    far_side = 1 - side_col
    owner_own = jnp.take_along_axis(send_rows, own_pick.reshape(NUM_PARTS, PEERS, HALO_ROWS * own_slots), axis=2)
    bound_src = jnp.concatenate([NODES_DEV + side_col * HALO_ROWS + cut_pick, owner_own.reshape(NUM_PARTS, PEERS, HALO_ROWS, own_slots)], axis=3)
    peer_orders = jnp.stack([jnp.roll(orders, -1, axis=0), jnp.roll(orders, 1, axis=0)], axis=1)
    cut_pos = (far_side * HALO_ROWS + cut_pick).reshape(NUM_PARTS, PEERS, HALO_ROWS * CUT_SLOTS)
    recv_cut = jnp.take_along_axis(peer_orders, cut_pos, axis=2).reshape(NUM_PARTS, PEERS, HALO_ROWS, CUT_SLOTS)
    recv_own = jnp.where(own_pick < HALO_ROWS, NODES_DEV + far_side * HALO_ROWS + own_pick, NODES_DEV + HALO_ROWS + far_side * HALO_ROWS + own_pick)
    recv_src = jnp.concatenate([recv_cut, recv_own], axis=3)
    weight_scale = DEGREE ** 0.5
    raw_w = jax.random.uniform(sub_keys[3], (NUM_PARTS, NODES_DEV, DEGREE), jnp.float32, 0.25, 1.75)
    cut_share = jax.random.uniform(sub_keys[4], (NUM_PARTS, PEERS, HALO_ROWS, 1), jnp.float32, 0.15, 0.35)
    bound_raw = raw_w[:, :band_rows].reshape(NUM_PARTS, PEERS, HALO_ROWS, DEGREE)
    cut_raw = bound_raw[:, :, :, :CUT_SLOTS]
    near_raw = bound_raw[:, :, :, CUT_SLOTS:]
    bound_w = jnp.concatenate([cut_raw * (cut_share * weight_scale / jnp.sum(cut_raw, axis=3, keepdims=True)), near_raw * ((1.0 - cut_share) * weight_scale / jnp.sum(near_raw, axis=3, keepdims=True))], axis=3)
    inner_raw = raw_w[:, band_rows:]
    inner_w = inner_raw * (weight_scale / jnp.sum(inner_raw, axis=2, keepdims=True))
    inner_src = jax.random.randint(sub_keys[5], (NUM_PARTS, NODES_DEV - band_rows, DEGREE), 0, NODES_DEV)
    inner_mark = (jax.random.randint(sub_keys[6], (NUM_PARTS, NODES_DEV - 2 * band_rows), 0, 8) == 0).astype(jnp.int32)
    src_sorted = jnp.concatenate([bound_src.reshape(NUM_PARTS, band_rows, DEGREE), inner_src], axis=1)
    w_sorted = jnp.concatenate([bound_w.reshape(NUM_PARTS, band_rows, DEGREE), inner_w], axis=1)
    mark_sorted = jnp.concatenate([jnp.ones((NUM_PARTS, 2 * band_rows), jnp.int32), inner_mark], axis=1)
    inverse = jnp.argsort(orders, axis=1)
    unsort = jax.vmap(lambda dev_rows, dev_order: dev_rows[dev_order])

    def to_receiver(per_sender):
        return jnp.stack([jnp.roll(per_sender[:, 1], -1, axis=0), jnp.roll(per_sender[:, 0], 1, axis=0)], axis=1)

    return {
        'send_idx': send_rows.reshape(NUM_PARTS * PEERS, 2 * HALO_ROWS),
        'edge_src': unsort(src_sorted, inverse).reshape(NUM_PARTS * NODES_DEV, DEGREE),
        'edge_w': unsort(w_sorted, inverse).reshape(NUM_PARTS * NODES_DEV, DEGREE),
        'halo_src': to_receiver(recv_src).reshape(NUM_PARTS * band_rows, DEGREE),
        'halo_w': to_receiver(bound_w).reshape(NUM_PARTS * band_rows, DEGREE),
        'label_mask': unsort(mark_sorted, inverse).reshape(NUM_PARTS * NODES_DEV),
    }


def setup_inputs(seed: int = 0) -> dict:
    root_key = jax.random.key(seed)
    key_feat, key_one, key_two, key_lab, key_graph = jax.random.split(root_key, 5)
    graph_parts = build_graph(key_graph)
    node_feats = jax.random.normal(key_feat, (NUM_PARTS * NODES_DEV, FEAT_IN), jnp.float32).astype(jnp.bfloat16)
    w_one = jax.random.normal(key_one, (FEAT_IN, HIDDEN), jnp.float32) * FEAT_IN ** -0.5
    w_two = jax.random.normal(key_two, (HIDDEN, CLASSES), jnp.float32) * HIDDEN ** -0.5
    labels = jax.random.randint(key_lab, (NUM_PARTS * NODES_DEV,), 0, CLASSES)
    return {'node_feats': node_feats, 'w_one': w_one, 'w_two': w_two, 'send_idx': graph_parts['send_idx'], 'edge_src': graph_parts['edge_src'], 'edge_w': graph_parts['edge_w'], 'halo_src': graph_parts['halo_src'], 'halo_w': graph_parts['halo_w'], 'labels': labels, 'label_mask': graph_parts['label_mask']}


def aggregate(buffer, src_rows, weights):
    return jnp.sum(buffer[src_rows].astype(jnp.float32) * weights[:, :, None], axis=1)


def reference(node_feats, w_one, w_two, send_idx, edge_src, edge_w, halo_src, halo_w, labels, label_mask):
    band_rows = PEERS * HALO_ROWS
    feats_dev = node_feats.reshape(NUM_PARTS, NODES_DEV, FEAT_IN)
    send_dev = send_idx.reshape(NUM_PARTS, PEERS, 2 * HALO_ROWS)
    src_dev = edge_src.reshape(NUM_PARTS, NODES_DEV, DEGREE)
    wts_dev = edge_w.reshape(NUM_PARTS, NODES_DEV, DEGREE)
    w_one_b = w_one.astype(jnp.bfloat16)
    w_two_b = w_two.astype(jnp.bfloat16)
    sent_rows = jax.vmap(lambda dev_rows, dev_index: dev_rows[dev_index])(feats_dev, send_dev)
    from_next = jnp.roll(sent_rows[:, 1], -1, axis=0)
    from_prev = jnp.roll(sent_rows[:, 0], 1, axis=0)
    full_buf = jnp.concatenate([feats_dev, from_next[:, :HALO_ROWS], from_prev[:, :HALO_ROWS], from_next[:, HALO_ROWS:], from_prev[:, HALO_ROWS:]], axis=1)

    def layer_one(operands):
        buf_rows, src_rows, wts_rows, hsrc_rows, hw_rows = operands
        z_own = aggregate(buf_rows, src_rows, wts_rows).astype(jnp.bfloat16)
        z_halo = aggregate(buf_rows, hsrc_rows, hw_rows).astype(jnp.bfloat16)
        y_own = jnp.dot(z_own, w_one_b, preferred_element_type=jnp.float32)
        y_halo = jnp.dot(z_halo, w_one_b, preferred_element_type=jnp.float32)
        return z_own, jnp.maximum(y_own, 0.0).astype(jnp.bfloat16), jnp.maximum(y_halo, 0.0).astype(jnp.bfloat16)

    z_one, h_two, h_halo = lax.map(layer_one, (full_buf, src_dev, wts_dev, halo_src.reshape(NUM_PARTS, band_rows, DEGREE), halo_w.reshape(NUM_PARTS, band_rows, DEGREE)))
    ext_two = jnp.concatenate([h_two, h_halo], axis=1)
    label_count = jnp.sum(label_mask.astype(jnp.float32))

    def layer_two(operands):
        buf_rows, src_rows, wts_rows, dev_labels, dev_mask = operands
        z_own = aggregate(buf_rows, src_rows, wts_rows).astype(jnp.bfloat16)
        dev_logits = jnp.dot(z_own, w_two_b, preferred_element_type=jnp.float32)
        onehot = (jnp.arange(CLASSES)[None, :] == dev_labels[:, None]).astype(jnp.float32)
        mark_rows = dev_mask.astype(jnp.float32) / label_count
        log_norm = jax.nn.logsumexp(dev_logits, axis=1)
        loss_part = jnp.sum(mark_rows * (log_norm - jnp.sum(dev_logits * onehot, axis=1)))
        grad_logits = ((jax.nn.softmax(dev_logits, axis=1) - onehot) * mark_rows[:, None]).astype(jnp.bfloat16)
        return z_own, loss_part, grad_logits

    z_two, loss_parts, grad_logits = lax.map(layer_two, (ext_two, src_dev, wts_dev, labels.reshape(NUM_PARTS, NODES_DEV), label_mask.reshape(NUM_PARTS, NODES_DEV)))
    loss_value = jnp.sum(loss_parts)
    grad_two = jnp.dot(z_two.reshape(NUM_PARTS * NODES_DEV, HIDDEN).T, grad_logits.reshape(NUM_PARTS * NODES_DEV, CLASSES), preferred_element_type=jnp.float32)

    def edge_grad(dev_grad, src_rows, wts_rows):
        grad_agg = jnp.dot(dev_grad, w_two_b.T, preferred_element_type=jnp.float32)
        contrib = (wts_rows[:, :, None] * grad_agg[:, None, :]).reshape(NODES_DEV * DEGREE, HIDDEN)
        return jax.ops.segment_sum(contrib, src_rows.reshape(NODES_DEV * DEGREE), num_segments=NODES_DEV + band_rows)

    halo_grad = lax.map(lambda operands: edge_grad(operands[0], operands[1], operands[2])[NODES_DEV:], (grad_logits, src_dev, wts_dev))
    back_next = jnp.roll(halo_grad[:, HALO_ROWS:], -1, axis=0)
    back_prev = jnp.roll(halo_grad[:, :HALO_ROWS], 1, axis=0)

    def layer_one_grad(operands):
        dev_grad, src_rows, wts_rows, send_part, next_part, prev_part, dev_hidden, dev_z = operands
        own_part = edge_grad(dev_grad, src_rows, wts_rows)[:NODES_DEV]
        grad_hidden = own_part.at[send_part[0, :HALO_ROWS]].add(next_part).at[send_part[1, :HALO_ROWS]].add(prev_part)
        grad_pre = jnp.where(dev_hidden > 0, grad_hidden, 0.0).astype(jnp.bfloat16)
        return jnp.dot(dev_z.T, grad_pre, preferred_element_type=jnp.float32)

    grad_one = jnp.sum(lax.map(layer_one_grad, (grad_logits, src_dev, wts_dev, send_dev, back_next, back_prev, h_two, z_one)), axis=0)
    return loss_value, grad_one, grad_two
```

```python
import functools

import jax
import jax.numpy as jnp
from jax import lax
from jax.experimental import pallas as pl
from jax.experimental.pallas import tpu as pltpu
from jax.sharding import PartitionSpec as P

MESH = pl.DeviceIdType.MESH
F32 = jnp.float32
BF16 = jnp.bfloat16
VMEM = pl.BlockSpec(memory_space=pltpu.VMEM)
SMEM = pl.BlockSpec(memory_space=pltpu.SMEM)
ANY = pl.BlockSpec(memory_space=pl.ANY)
CLASSES = 47
LANES = 128
CHUNK = 256


def wrap(value, size):
    return lax.rem(value + size, size)


def remote(src, dst, send_sem, recv_sem, dev):
    return pltpu.make_async_remote_copy(src_ref=src, dst_ref=dst, send_sem=send_sem, recv_sem=recv_sem, device_id=(dev,), device_id_type=MESH)


def enter(peers):
    barrier = pltpu.get_barrier_semaphore()
    for dev in peers:
        pl.semaphore_signal(barrier, inc=1, device_id=(dev,), device_id_type=MESH)


def entered(peers):
    pl.semaphore_wait(pltpu.get_barrier_semaphore(), len(peers))


def line_peers(me):
    block, in_x = me // 8, lax.rem(me, 8)
    plane, in_y = me // 32, lax.rem(block, 4)
    along_x = [block * 8 + lax.rem(in_x + d, 8) for d in range(1, 8)]
    along_y = [plane * 32 + lax.rem(in_y + d, 4) * 8 + in_x for d in range(1, 4)]
    along_z = [lax.rem(plane + d, 4) * 32 + in_y * 8 + in_x for d in range(1, 4)]
    return in_x, in_y, plane, along_x, along_y, along_z


def spread(slots, mine, peers, send_sem, recv_sem):
    copies = []
    for d, dev in enumerate(peers):
        copies.append(remote(slots.at[mine], slots.at[mine], send_sem.at[d], recv_sem.at[d], dev))
        copies[-1].start()
    return copies


def settle(copies):
    for copy in copies:
        copy.wait()


def slot_sum(slots):
    total = slots[0]
    for i in range(1, slots.shape[0]):
        total = total + slots[i]
    return total


def pick_rows(send_idx, src, stage, halo):
    for side in range(2):
        for j in range(halo):
            stage[pl.ds(side * halo + j, 1), :] = src[pl.ds(send_idx[side, j], 1), :]


def feats_kernel(halo, send_idx, feats_t, mask, x_out, send_buf, count_out, wide, stage):
    feats, own = feats_t.shape
    mask_f = mask[...].astype(F32)
    count_out[...] = functools.reduce(lambda a, b: a + b, [mask_f[8 * i:8 * i + 8] for i in range(mask.shape[0] // 8)])
    wide[pl.ds(0, feats), :] = feats_t[...].astype(F32)
    wide[pl.ds(feats, LANES - feats), :] = jnp.zeros((LANES - feats, own), F32)
    for b in range(own // LANES):
        x_out[pl.ds(b * LANES, LANES), :] = wide[:, b * LANES:(b + 1) * LANES].T
    pick_rows(send_idx, x_out, stage, halo)
    send_buf[...] = stage[...].astype(BF16)


def swap_kernel(halo, num_parts, send_buf, count_in, recv_buf, count_out, counts, sem_s, sem_r, csem_s, csem_r):
    me = lax.axis_index('graph')
    nxt, prv = wrap(me + 1, num_parts), wrap(me - 1, num_parts)
    in_x, _, _, along_x, _, _ = line_peers(me)
    peers = [nxt, prv] + along_x
    enter(peers)
    counts[in_x] = count_in[...]
    entered(peers)
    copies = [remote(send_buf.at[pl.ds(0, halo)], recv_buf.at[pl.ds(halo, halo)], sem_s.at[0], sem_r.at[0], nxt),
              remote(send_buf.at[pl.ds(halo, halo)], recv_buf.at[pl.ds(0, halo)], sem_s.at[1], sem_r.at[1], prv)]
    for copy in copies:
        copy.start()
    settle(spread(counts, in_x, along_x, csem_s, csem_r))
    count_out[...] = slot_sum(counts)
    settle(copies)


def hidden_kernel(halo, num_parts, send_buf, count_in, recv_buf, count_out, count_y, count_z, sem_s, sem_r, csem_s, csem_r):
    me = lax.axis_index('graph')
    nxt, prv = wrap(me + 1, num_parts), wrap(me - 1, num_parts)
    _, in_y, in_z, _, along_y, along_z = line_peers(me)
    peers = [nxt, prv] + along_y + along_z
    enter(peers)
    count_y[in_y] = count_in[...]
    entered(peers)
    copies = [remote(send_buf.at[pl.ds(0, halo)], recv_buf.at[pl.ds(halo, halo)], sem_s.at[0], sem_r.at[0], nxt),
              remote(send_buf.at[pl.ds(halo, halo)], recv_buf.at[pl.ds(0, halo)], sem_s.at[1], sem_r.at[1], prv)]
    for copy in copies:
        copy.start()
    settle(spread(count_y, in_y, along_y, csem_s.at[0], csem_r.at[0]))
    count_z[in_z] = slot_sum(count_y)
    settle(spread(count_z, in_z, along_z, csem_s.at[1], csem_r.at[1]))
    count_out[...] = jnp.full(count_out.shape, jnp.sum(slot_sum(count_z)), F32)
    settle(copies)


def grads_kernel(num_parts, halo, send_buf, recv_buf, sem_s, sem_r):
    me = lax.axis_index('graph')
    nxt, prv = wrap(me + 1, num_parts), wrap(me - 1, num_parts)
    enter([nxt, prv])
    entered([nxt, prv])
    copies = [remote(send_buf.at[pl.ds(0, halo)], recv_buf.at[pl.ds(halo, halo)], sem_s.at[0], sem_r.at[0], nxt),
              remote(send_buf.at[pl.ds(halo, halo)], recv_buf.at[pl.ds(0, halo)], sem_s.at[1], sem_r.at[1], prv)]
    for copy in copies:
        copy.start()
    settle(copies)


def reduce_kernel(mine, whole, by_x, by_y, by_z, sem_s, sem_r):
    me = lax.axis_index('graph')
    in_x, in_y, in_z, along_x, along_y, along_z = line_peers(me)
    peers = along_x + along_y + along_z
    enter(peers)
    by_x[in_x] = mine[in_x]
    entered(peers)
    copies = []
    for d, dev in enumerate(along_x):
        copies.append(remote(mine.at[lax.rem(in_x + d + 1, 8)], by_x.at[in_x], sem_s.at[0, d], sem_r.at[0, d], dev))
        copies[-1].start()
    settle(copies)
    by_y[in_y] = slot_sum(by_x)
    settle(spread(by_y, in_y, along_y, sem_s.at[1], sem_r.at[1]))
    by_z[in_z] = slot_sum(by_y)
    settle(spread(by_z, in_z, along_z, sem_s.at[2], sem_r.at[2]))
    whole[in_x] = slot_sum(by_z)
    settle(spread(whole, in_x, along_x, sem_s.at[3], sem_r.at[3]))


def packed_places(feats, classes, hid):
    places, at = [], 0
    for rows in (feats, classes):
        for col in range(0, hid, LANES):
            places.append((at, rows, col))
            at += -(-rows // 8) * 8
    return places, at


def finish_kernel(whole, count, out_one, out_two, out_loss):
    feats, hid = out_one.shape
    places, at = packed_places(feats, out_two.shape[0], hid)
    half = len(places) // 2
    for ref, spots in ((out_one, places[:half]), (out_two, places[half:])):
        for start, rows, col in spots:
            ref[:, col:col + LANES] = whole[pl.ds(start, rows), :]
    out_loss[...] = jnp.full(out_loss.shape, jnp.sum(whole[pl.ds(at, 8), :]), F32) / count[...]


def columns(w3, t, *more):
    parts = [w3[t]] + [ref[t].astype(F32) for ref in more]
    parts.append(jnp.zeros((8 - 4 - len(more), LANES), F32))
    return jnp.concatenate(parts, axis=0).T


def layer_one_kernel(halo, src_any, src_v, x_any, x_halo, w3, w_one, send_idx, z_out, h_out, src_out, hsend, *scratch):
    idx, slots = scratch[0:2], (scratch[2:6], scratch[6:10])
    stage, x_buf, sem, xsem = scratch[10:14]
    own = z_out.shape[0]
    pull = pltpu.make_async_copy(x_any, x_buf.at[pl.ds(0, own)], xsem)
    pull.start()
    steps = own // CHUNK
    src_out[...] = src_v[...] * 2

    def fetch(c, b):
        return pltpu.make_async_copy(src_any.at[pl.ds(2 * c, 2)], idx[b], sem.at[b])

    def gather(b):
        for k in range(4):
            for t in range(2):
                for j in range(LANES):
                    slots[b][k][pl.ds(t * LANES + j, 1), :] = x_buf[pl.ds(idx[b][t, k, j], 1), :]

    def dense(c, b):
        r0 = pl.multiple_of(c * CHUNK, CHUNK)
        blocks = []
        for t in range(2):
            cols = columns(w3, 2 * c + t)
            sl = pl.ds(t * LANES, LANES)
            acc = slots[b][0][sl, :] * cols[:, 0:1]
            for k in range(1, 4):
                acc = acc + slots[b][k][sl, :] * cols[:, k:k + 1]
            blocks.append(acc.astype(BF16))
        z = jnp.concatenate(blocks, axis=0)
        z_out[pl.ds(r0, CHUNK), :] = z
        y = jnp.dot(z, w_one[...], preferred_element_type=F32)
        h = jnp.maximum(y, 0.0).astype(BF16).astype(F32)
        h_out[pl.ds(2 * r0, CHUNK, stride=2), :] = h[:, :LANES]
        h_out[pl.ds(2 * r0 + 1, CHUNK, stride=2), :] = h[:, LANES:]

    for b in range(2):
        fetch(b, b).start()
    for k in range(4):
        slots[1][k][...] = jnp.zeros(slots[1][k].shape, F32)
    x_buf[pl.ds(own, 2 * halo), :] = x_halo[...].astype(F32)
    pull.wait()

    def body(g, carry):
        for b in range(2):
            c = g * 2 + b
            fetch(c, b).wait()
            gather(b)
            dense(jnp.maximum(c - 1, 0), 1 - b)

            @pl.when(c + 2 < steps)
            def _():
                fetch(c + 2, b).start()
        return carry

    lax.fori_loop(0, steps // 2, body, 0)
    dense(steps - 1, 1)
    for side in range(2):
        for j in range(halo):
            i = pl.multiple_of(send_idx[side, j] * 2, 2)
            stage[pl.ds(2 * (side * halo + j), 2), :] = h_out[pl.ds(i, 2), :]
    hsend[...] = stage[...].astype(BF16)


def layer_two_kernel(src_any, src2_any, h_any, h_halo, w3, labels, mask, w_two, count, p_out, grad_two, loss, *scratch):
    fwd_idx, bwd_idx = scratch[0:2], scratch[2:4]
    slots = (scratch[4:8], scratch[8:12])
    terms = (scratch[12:16], scratch[16:20])
    sums = scratch[20:28]
    h_buf, fsem, bsem, hsem = scratch[28:32]
    own = w3.shape[0] * LANES
    steps = own // CHUNK
    pull = pltpu.make_async_copy(h_any, h_buf.at[pl.ds(0, 2 * own)], hsem)
    pull.start()

    def fetch(c, b):
        return pltpu.make_async_copy(src2_any.at[pl.ds(2 * c, 2)], fwd_idx[b], fsem.at[b])

    def refetch(c, b):
        return pltpu.make_async_copy(src_any.at[pl.ds(2 * c, 2)], bwd_idx[b], bsem.at[b])

    def gather(b):
        for k in range(4):
            for t in range(2):
                for j in range(LANES):
                    i = pl.multiple_of(fwd_idx[b][t, k, j], 2)
                    slots[b][k][pl.ds(2 * (t * LANES + j), 2), :] = h_buf[pl.ds(i, 2), :]

    def dense(c, b, valid):
        zs, lab, scale, marks = [], [], [], []
        cols_t = []
        for t in range(2):
            cols = columns(w3, 2 * c + t, labels, mask)
            cols_t.append(cols)
            halves = []
            for half in range(2):
                sl = pl.ds(2 * t * LANES + half, LANES, stride=2)
                acc = slots[b][0][sl, :] * cols[:, 0:1]
                for k in range(1, 4):
                    acc = acc + slots[b][k][sl, :] * cols[:, k:k + 1]
                halves.append(acc.astype(BF16))
            zs.append(jnp.concatenate(halves, axis=1))
        z = jnp.concatenate(zs, axis=0)
        logits = jnp.dot(z, w_two[...], preferred_element_type=F32)
        lane = lax.broadcasted_iota(jnp.int32, (CHUNK, LANES), 1)
        lab = jnp.concatenate([cols[:, 4:5] for cols in cols_t], axis=0).astype(jnp.int32)
        marks = jnp.where(valid, jnp.concatenate([cols[:, 5:6] for cols in cols_t], axis=0), 0.0)
        hot = lane == lab
        shown = jnp.where(lane < CLASSES, logits, -1e30)
        top = jnp.max(shown, axis=1, keepdims=True)
        expo = jnp.exp(shown - top)
        norm = jnp.sum(expo, axis=1, keepdims=True)
        picked = jnp.sum(jnp.where(hot, logits, 0.0), axis=1, keepdims=True)
        row_loss = marks * (jnp.log(norm) + top - picked)
        loss[...] += jnp.full(loss.shape, jnp.sum(row_loss), F32) * first_cell
        grad = ((expo / norm - jnp.where(hot, 1.0, 0.0)) * (marks / count[0, 0])).astype(BF16)
        grad_two[...] += lax.dot_general(grad, z, (((0,), (0,)), ((), ())), preferred_element_type=F32)
        wide = grad.astype(F32)
        for t in range(2):
            sl = pl.ds(t * LANES, LANES)
            for k in range(4):
                terms[b][k][sl, :] = wide[t * LANES:(t + 1) * LANES] * cols_t[t][:, k:k + 1]

    def scatter(b):
        for t in range(2):
            for j in range(0, LANES, 2):
                where, had = [], []
                for u in range(2):
                    for k in range(4):
                        where.append(pl.ds(bwd_idx[b][t, k, j + u], 1))
                for u in range(2):
                    for k in range(4):
                        had.append(sums[4 * u + k][where[4 * u + k], :] + terms[b][k][pl.ds(t * LANES + j + u, 1), :])
                for u in range(2):
                    for k in range(4):
                        sums[4 * u + k][where[4 * u + k], :] = had[4 * u + k]

    cell = (lax.broadcasted_iota(jnp.int32, loss.shape, 0) == 0) & (lax.broadcasted_iota(jnp.int32, loss.shape, 1) == 0)
    first_cell = jnp.where(cell, 1.0, 0.0).astype(F32)
    for b in range(2):
        fetch(b, b).start()
        refetch(0, b).start()
    for acc in sums:
        acc[...] = jnp.zeros(acc.shape, F32)
    for k in range(4):
        slots[1][k][...] = jnp.zeros(slots[1][k].shape, F32)
        for b in range(2):
            terms[b][k][...] = jnp.zeros(terms[b][k].shape, F32)
    loss[...] = jnp.zeros(loss.shape, F32)
    grad_two[...] = jnp.zeros(grad_two.shape, F32)
    h_buf[pl.ds(2 * own, h_halo.shape[0]), :] = h_halo[...].astype(F32)
    pull.wait()

    def body(g, carry):
        for b in range(2):
            c = g * 2 + b
            fetch(c, b).wait()
            refetch(c, b).wait()
            gather(b)
            dense(jnp.maximum(c - 1, 0), 1 - b, c > 0)
            scatter(b)
            refetch(c, b).start()

            @pl.when(c + 2 < steps)
            def _():
                fetch(c + 2, b).start()
        return carry

    lax.fori_loop(0, steps // 2, body, 0)
    refetch(steps - 2, 0).wait()
    dense(steps - 1, 1, True)
    scatter(0)
    refetch(steps - 1, 1).wait()
    scatter(1)
    p_out[...] = functools.reduce(lambda a, b: a + b, [acc[...] for acc in sums])


def layer_one_grad_kernel(halo, feats, classes, send_idx, p_buf, back, z_one, h_any, w_stack, grad_two, loss, packed, grad_one, p_own, h_buf, sem):
    own = z_one.shape[0]
    pull = pltpu.make_async_copy(h_any, h_buf, sem)
    pull.start()
    p_own[...] = p_buf[pl.ds(0, own), :]
    for side in range(2):
        for j in range(0, halo, 16):
            rows = [send_idx[side, j + u] for u in range(16)]
            new = [p_own[pl.ds(rows[u], 1), :] + back[pl.ds(side * halo + j + u, 1), :] for u in range(16)]
            for u in range(16):
                p_own[pl.ds(rows[u], 1), :] = new[u]
    grad_one[...] = jnp.zeros(grad_one.shape, F32)
    pull.wait()

    def body(c, carry):
        r0 = pl.multiple_of(c * CHUNK, CHUNK)
        p = p_own[pl.ds(r0, CHUNK), :]
        high = p.astype(BF16)
        rest = p - high.astype(F32)
        mid = rest.astype(BF16)
        low = (rest - mid.astype(F32)).astype(BF16)
        both = high.astype(F32) + pltpu.roll(mid.astype(F32), 64, 1)
        lhs = jnp.concatenate([both.astype(BF16), low], axis=1)
        hidden = jnp.dot(lhs, w_stack[...], preferred_element_type=F32)
        h = jnp.concatenate([h_buf[pl.ds(2 * r0 + half, CHUNK, stride=2), :] for half in range(2)], axis=1)
        grad = jnp.where(h > 0, hidden, 0.0).astype(BF16)
        grad_one[...] += lax.dot_general(z_one[pl.ds(r0, CHUNK), :], grad, (((0,), (0,)), ((), ())), preferred_element_type=F32)
        return carry

    lax.fori_loop(0, own // CHUNK, body, 0)
    places, at = packed_places(feats, classes, grad_one.shape[1])
    half = len(places) // 2
    for ref, spots in ((grad_one, places[:half]), (grad_two, places[half:])):
        for start, rows, col in spots:
            rows = -(-rows // 8) * 8
            packed[pl.ds(start, rows), :] = ref[pl.ds(0, rows), col:col + LANES]
    packed[pl.ds(at, 8), :] = loss[...]
    packed[pl.ds(at + 8, packed.shape[0] - at - 8), :] = jnp.zeros((packed.shape[0] - at - 8, LANES), F32)


def params(mib, collective_id=None):
    if collective_id is None:
        return pltpu.CompilerParams(vmem_limit_bytes=mib * 2 ** 20)
    return pltpu.CompilerParams(vmem_limit_bytes=mib * 2 ** 20, collective_id=collective_id, has_side_effects=True)


def solution(mesh):
    num_parts = mesh.shape['graph']
    row_spec = P('graph', None)

    def device_step(node_feats, w_one, w_two, send_idx, edge_src, edge_w, labels, label_mask):
        own, feats = node_feats.shape
        hid, classes = w_two.shape
        halo = send_idx.shape[1] // 2
        blocks = own // LANES
        buf = own + 2 * halo
        dma = pltpu.SemaphoreType.DMA
        shape = jax.ShapeDtypeStruct
        src3 = edge_src.T.reshape(4, blocks, LANES).transpose(1, 0, 2)
        w3 = edge_w.T.reshape(4, blocks, LANES).transpose(1, 0, 2)
        labels3 = labels.reshape(blocks, 1, LANES)
        mask3 = label_mask.reshape(blocks, 1, LANES)
        w_one_b = jnp.pad(w_one.astype(BF16), ((0, LANES - feats), (0, 0)))
        w_two_b = jnp.pad(w_two.astype(BF16), ((0, 0), (0, LANES - classes)))
        w_two_t = jnp.pad(w_two.astype(BF16).T, ((0, 64 - classes), (0, 0)))
        w_stack = jnp.concatenate([w_two_t, w_two_t, w_two_t, jnp.zeros_like(w_two_t)], axis=0)
        tile = shape((8, LANES), F32)

        x_own, x_send, count_own = pl.pallas_call(
            functools.partial(feats_kernel, halo), name='feats',
            out_shape=(shape((own, LANES), F32), shape((2 * halo, LANES), BF16), tile),
            in_specs=[SMEM, VMEM, VMEM], out_specs=[VMEM] * 3,
            scratch_shapes=[pltpu.VMEM((LANES, own), F32), pltpu.VMEM((2 * halo, LANES), F32)],
            compiler_params=params(16),
        )(send_idx, node_feats.T, label_mask.reshape(blocks, LANES))

        x_halo, count_x = pl.pallas_call(
            functools.partial(swap_kernel, halo, num_parts), name='swap_feats',
            out_shape=(shape((2 * halo, LANES), BF16), tile),
            in_specs=[VMEM, VMEM], out_specs=[VMEM, VMEM],
            scratch_shapes=[pltpu.VMEM((8, 8, LANES), F32), dma((2,)), dma((2,)), dma((7,)), dma((7,))],
            compiler_params=params(4, 0),
        )(x_send, count_own)

        chunk_idx = pltpu.SMEM((2, 4, LANES), jnp.int32)
        z_one, h_two, src2, h_send = pl.pallas_call(
            functools.partial(layer_one_kernel, halo), name='layer_one',
            out_shape=(shape((own, LANES), BF16), shape((2 * own, LANES), F32), shape(src3.shape, jnp.int32), shape((4 * halo, LANES), BF16)),
            in_specs=[ANY, VMEM, ANY, VMEM, VMEM, VMEM, SMEM], out_specs=[VMEM] * 4,
            scratch_shapes=[chunk_idx] * 2 + [pltpu.VMEM((CHUNK, LANES), F32)] * 8 + [pltpu.VMEM((4 * halo, LANES), F32), pltpu.VMEM((buf, LANES), F32), dma((2,)), dma],
            compiler_params=params(24),
        )(src3, src3, x_own, x_halo, w3, w_one_b, send_idx)

        h_halo, count = pl.pallas_call(
            functools.partial(hidden_kernel, 2 * halo, num_parts), name='hidden',
            out_shape=(shape((4 * halo, LANES), BF16), tile),
            in_specs=[VMEM, VMEM], out_specs=[VMEM, VMEM],
            scratch_shapes=[pltpu.VMEM((4, 8, LANES), F32)] * 2 + [dma((2,)), dma((2,)), dma((2, 3)), dma((2, 3))],
            compiler_params=params(8, 1),
        )(h_send, count_x)

        p_buf, grad_two, loss = pl.pallas_call(
            layer_two_kernel, name='layer_two',
            out_shape=(shape((buf, LANES), F32), shape((LANES, hid), F32), tile),
            in_specs=[ANY, ANY, ANY] + [VMEM] * 6, out_specs=[VMEM] * 3,
            scratch_shapes=[chunk_idx] * 4 + [pltpu.VMEM((2 * CHUNK, LANES), F32)] * 8 + [pltpu.VMEM((CHUNK, LANES), F32)] * 8 + [pltpu.VMEM((buf, LANES), F32)] * 8 + [pltpu.VMEM((2 * buf, LANES), F32), dma((2,)), dma((2,)), dma],
            compiler_params=params(48),
        )(src3, src2, h_two, h_halo, w3, labels3, mask3, w_two_b, count)

        back = pl.pallas_call(
            functools.partial(grads_kernel, num_parts, halo), name='grads',
            out_shape=shape((2 * halo, LANES), F32),
            in_specs=[VMEM], out_specs=VMEM,
            scratch_shapes=[dma((2,)), dma((2,))],
            compiler_params=params(8, 2),
        )(p_buf[own:])

        rows = packed_places(feats, classes, hid)[1] + 8
        part = -(-rows // 64) * 8
        packed = pl.pallas_call(
            functools.partial(layer_one_grad_kernel, halo, feats, classes), name='layer_one_grad',
            out_shape=shape((8 * part, LANES), F32),
            in_specs=[SMEM, VMEM, VMEM, VMEM, ANY, VMEM, VMEM, VMEM], out_specs=VMEM,
            scratch_shapes=[pltpu.VMEM((LANES, hid), F32), pltpu.VMEM((own, LANES), F32), pltpu.VMEM((2 * own, LANES), F32), dma],
            compiler_params=params(24),
        )(send_idx, p_buf, back, z_one, h_two, w_stack, grad_two, loss)

        whole = pl.pallas_call(
            reduce_kernel, name='reduce',
            out_shape=shape((8, part, LANES), F32),
            in_specs=[VMEM], out_specs=VMEM,
            scratch_shapes=[pltpu.VMEM((8, part, LANES), F32), pltpu.VMEM((4, part, LANES), F32), pltpu.VMEM((4, part, LANES), F32), dma((4, 7)), dma((4, 7))],
            compiler_params=params(4, 3),
        )(packed.reshape(8, part, LANES))

        out_one, out_two, out_loss = pl.pallas_call(
            finish_kernel, name='finish',
            out_shape=(shape((feats, hid), F32), shape((classes, hid), F32), tile),
            in_specs=[VMEM] * 2, out_specs=[VMEM] * 3,
            compiler_params=params(4),
        )(whole.reshape(8 * part, LANES), count)
        return out_loss[0, 0], out_one, out_two.T

    mapped = jax.shard_map(device_step, mesh=mesh, in_specs=(row_spec, P(), P(), row_spec, row_spec, row_spec, P('graph'), P('graph')), out_specs=(P(), P(), P()), check_vma=False)

    def program(node_feats, w_one, w_two, send_idx, edge_src, edge_w, halo_src, halo_w, labels, label_mask):
        return mapped(node_feats, w_one, w_two, send_idx, edge_src, edge_w, labels, label_mask)

    return program
```
